512 devices in a mesh: users: 32 (over z, y_hi, core), items: 16 (over y_lo, x).
Axes of the slice: x: 4, y: 8 (y_hi: 2, y_lo: 4; y = y_hi * 4 + y_lo), z: 8, core: 2. Of those that a mesh axis runs over, the one named last changes fastest.
Arguments:
- prefs: int32 [32768, 16384], P('users', 'items'), may hold values from 0 to 4
- item_weight: float32 [16384], P('items'), may hold values from 0.05 to 1.35
- clip_units: int32 [32768], P('users'), may hold values from 100 to 999
- user_emb: float32 [32768, 128], P(('users', 'items')), may hold values from -0.6 to 0.6
- user_acc: float32 [32768, 128], P(('users', 'items')), may hold values from 100 to 3000
- item_emb: float32 [16384, 128], P(('items', 'users')), may hold values from -0.6 to 0.6
- item_acc: float32 [16384, 128], P(('items', 'users')), may hold values from 100 to 3000
- noise: int32 [16384, 128], P(('items', 'users')), may hold values from -1000 to 1000
Outputs:
- new_user_emb: float32 [32768, 128], P(('users', 'items'))
- new_user_acc: float32 [32768, 128], P(('users', 'items'))
- new_item_emb: float32 [16384, 128], P(('items', 'users'))
- new_item_acc: float32 [16384, 128], P(('items', 'users'))
The draws below stay inside these ranges and needn't reach their ends.
All inputs are finite; a program needn't handle non-finite values.
Results may differ from the reference program's by a relative error of at most 0.0003.
Values sent between devices are 32-bit elements; how exact they have to be, the bound alone decides.
No kernel may reach another device: no remote copies, remote signals or barrier semaphores. Data moves between devices by JAX's collectives and lax.ppermute only.
A program may use at most 64 MiB of HBM per device.

```python
import math
import jax
import jax.numpy as jnp
from jax import lax

K = 128
UD = 1024
NU = 32768
NI = 16384
N_USERS = 32


def draw_item_weight(key, part):
    position = jnp.arange(NI, dtype=jnp.float32) / NI
    base_rate = 0.1 * jnp.exp(jnp.log(9.0) * position)
    jitter = jax.random.uniform(key, (NI,), jnp.float32, 0.7, 1.3)
    return (base_rate * jitter).astype(jnp.float32)


def set_ends(drawn, key, least, top_value):
    shape = drawn.shape
    place = [jax.random.randint(jax.random.fold_in(key, axis), (), 0, shape[axis]) for axis in range(len(shape))]
    drawn = drawn.at[tuple(place)].set(least)
    longest = shape.index(max(shape))
    place[longest] = (place[longest] + 1) % shape[longest]
    return drawn.at[tuple(place)].set(top_value)


def shard_levels(stream_key, extent, cuts, low, high):
    level, own = 1.0, jax.random.fold_in(stream_key, 6)
    for dim, shards_of in cuts:
        steps = jnp.exp(jax.random.uniform(jax.random.fold_in(own, dim), (shards_of,), jnp.float32, low / len(cuts), high / len(cuts)))
        level = level * jnp.repeat(steps, extent[dim] // shards_of).reshape([-1 if axis == dim else 1 for axis in range(len(extent))])
    return level


def centred(rng, shape, spread, reach, shards=(), kind=jnp.bfloat16):
    level = shard_levels(rng, shape, shards, -0.22, 0.18) if shards else 1.0
    values = jax.random.normal(rng, shape, jnp.float32) * spread * level
    return jnp.minimum(jnp.maximum(values, -reach), reach).astype(kind)


def setup_inputs(seed: int = 0) -> dict:
    key_list = jax.random.split(jax.random.key(seed), 9)
    prefs = set_ends(jax.random.randint(key_list[0], (NU, NI), 0, 5), jax.random.fold_in(key_list[0], 1), 0, 4).astype(jnp.int32)
    item_weight = draw_item_weight(jax.random.fold_in(key_list[8], 71), 0)
    clip_units = set_ends(jax.random.randint(key_list[2], (NU,), 100, 1000), jax.random.fold_in(key_list[2], 1), 100, 999).astype(jnp.int32)
    user_emb = centred(key_list[3], (NU, K), 0.1, 0.6, ((0, 512),), jnp.float32)
    user_acc = jnp.clip(jnp.exp(math.log(3000.0) - 3.4011974 * jax.random.uniform(key_list[4], (NU, K), jnp.float32) ** shard_levels(key_list[4], (NU, K), ((0, 512),), -0.2, 0.2)), 100.0, 3000.0)
    item_emb = centred(key_list[5], (NI, K), 0.1, 0.6, ((0, 512),), jnp.float32)
    item_acc = jnp.clip(jnp.exp(math.log(3000.0) - 3.4011974 * jax.random.uniform(key_list[6], (NI, K), jnp.float32) ** shard_levels(key_list[6], (NI, K), ((0, 512),), -0.2, 0.2)), 100.0, 3000.0)
    noise = set_ends(jax.random.randint(key_list[7], (NI, K), -1000, 1001), jax.random.fold_in(key_list[7], 1), -1000, 1000).astype(jnp.int32)
    return {"prefs": prefs, "item_weight": item_weight, "clip_units": clip_units, "user_emb": user_emb, "user_acc": user_acc, "item_emb": item_emb, "item_acc": item_acc, "noise": noise}


noise_step = 0.05
learn_rate = 0.5

def reference(prefs, item_weight, clip_units, user_emb, user_acc, item_emb, item_acc, noise):
    precise = lax.Precision.HIGHEST
    pref_blocks = prefs.reshape(N_USERS, UD, NI)
    user_blocks = user_emb.reshape(N_USERS, UD, K)
    clip_blocks = clip_units.reshape(N_USERS, UD)
    bound_scale = 0.001 * jnp.sqrt(jnp.float32(NI * K))

    def visit(totals, inputs):
        pref_rows, user_rows, clip_rows = inputs
        predicted = lax.dot_general(user_rows, item_emb, (((1,), (1,)), ((), ())), precision=precise, preferred_element_type=jnp.float32)
        target = jnp.where(pref_rows > 0, 1.0, 0.0).astype(jnp.float32)
        confidence = 1.0 + item_weight[None, :] * pref_rows.astype(jnp.float32)
        weighted = -2.0 * confidence * (target - predicted)
        resid_sq = lax.optimization_barrier(jnp.sum(weighted * weighted, axis=1))
        user_sq = lax.optimization_barrier(jnp.sum(user_rows * user_rows, axis=1))
        factor = jnp.minimum(1.0, clip_rows.astype(jnp.float32) * bound_scale / jnp.sqrt(resid_sq * user_sq + 1e-06))
        gradient = jnp.dot(weighted, item_emb, precision=precise, preferred_element_type=jnp.float32)
        scaled = user_rows * factor[:, None]
        totals = totals + lax.dot_general(weighted, scaled, (((0,), (0,)), ((), ())), precision=precise, preferred_element_type=jnp.float32)
        return (totals, gradient)
    initial = jnp.zeros((NI, K), jnp.float32)
    item_sum, user_parts = lax.scan(visit, initial, (pref_blocks, user_blocks, clip_blocks))
    user_grad = user_parts.reshape(NU, K)
    item_grad = item_sum + noise_step * noise.astype(jnp.float32)
    new_user_acc = user_acc + user_grad * user_grad
    new_user_emb = user_emb - learn_rate * user_grad / jnp.sqrt(new_user_acc)
    new_item_acc = item_acc + item_grad * item_grad
    new_item_emb = item_emb - learn_rate * item_grad / jnp.sqrt(new_item_acc)
    return (new_user_emb, new_user_acc, new_item_emb, new_item_acc)
```

```python
import jax
import jax.numpy as jnp
from jax import lax
from jax.experimental import pallas as pl
from jax.experimental.pallas import tpu as pltpu
from jax.sharding import Mesh, PartitionSpec as P

noise_step = 0.05
learn_rate = 0.5
lanes = 128
f32 = jnp.float32
bf16 = jnp.bfloat16

names = ("z", "half", "core", "run", "x")
sizes = (8, 2, 2, 4, 4)
user_axes = names[:3]
item_axes = names[3:]
chip_axes = names[:2]

whole = pl.BlockSpec(memory_space=pltpu.VMEM)


def halves(value):
    high = value.astype(bf16)
    return high, (value - high.astype(f32)).astype(bf16)


def product(left, right):
    return jnp.dot(left, right, preferred_element_type=f32)


def cost(flops):
    return pl.CostEstimate(flops=flops, bytes_accessed=1 << 20, transcendentals=0)


def block_kernel(
    user_ref, item_ref, far_ref, rate_ref, high_ref, low_ref, sent_ref, turned_ref, norm_ref, pair_ref, rest_ref, tall_ref, prefs_ref, ready
):
    parts, steps, piece, width = user_ref.shape
    users, items = prefs_ref.shape
    rows = parts * piece
    tile = 2 * lanes
    blocks = [slice(step * rows, (step + 1) * rows) for step in range(steps)]
    copies = [pltpu.make_async_copy(far_ref.at[span], prefs_ref.at[span], ready.at[step]) for step, span in enumerate(blocks)]
    for copy in copies:
        copy.start()
    cores, _, bit, _ = item_ref.shape
    per = lanes // (cores * bit)
    for part in range(items // lanes):
        place = slice(part * lanes, (part + 1) * lanes)
        together = [item_ref[core, part * per + line] for line in range(per) for core in range(cores)]
        value = jnp.concatenate(together, axis=0)
        high, low = halves(value)
        tall_ref[place, :width] = high
        tall_ref[place, width:] = low
        high, low = halves(value.T)
        pair_ref[:width, place] = high
        pair_ref[width:, place] = high
        rest_ref[:, place] = low
    for step, span in enumerate(blocks):
        user = user_ref[:, step].reshape(rows, width)
        user_high, user_low = halves(user)
        both = jnp.concatenate([user_high, user_low], axis=1)
        squares = jnp.zeros((rows, lanes), f32)
        copies[step].wait()
        for part in range(items // tile):
            place = slice(part * tile, (part + 1) * tile)
            predicted = product(both, pair_ref[:, place]) + product(user_high, rest_ref[:, place])
            level = prefs_ref[span, place].astype(f32)
            confidence = 2.0 + 2.0 * rate_ref[:, place] * level
            weighted = confidence * (predicted - jnp.where(level > 0, 1.0, 0.0))
            high_ref[span, place], low_ref[span, place] = halves(weighted)
            square = weighted * weighted
            squares = squares + square[:, :lanes] + square[:, lanes:]
        wide = product(high_ref[span, :], tall_ref[...])
        gradient = wide[:, :width] + wide[:, width:] + product(low_ref[span, :], tall_ref[:, :width])
        for part in range(parts):
            sent_ref[part, step * piece : (step + 1) * piece, :] = gradient[part * piece : (part + 1) * piece, :]
        for part in range(rows // lanes):
            place = slice(part * lanes, (part + 1) * lanes)
            row = step * (rows // lanes) + part
            turned = user[place, :].T
            turned_ref[:, row * lanes : (row + 1) * lanes] = turned
            norm_ref[row : row + 1, :] = jnp.sum(turned * turned, axis=0, keepdims=True)
            total = jnp.sum(squares[place, :].T, axis=0, keepdims=True)
            for other in range(parts):
                sent_ref[other, steps * piece + row : steps * piece + row + 1, :] = total


def block(user_rows, item_rows, prefs, rate):
    parts, steps, piece, width = user_rows.shape
    users, items = prefs.shape
    groups = users // lanes
    return pl.pallas_call(
        block_kernel,
        in_specs=[whole, whole, pl.BlockSpec(memory_space=pltpu.HBM), whole],
        out_specs=[whole] * 5,
        out_shape=[
            jax.ShapeDtypeStruct((users, items), bf16),
            jax.ShapeDtypeStruct((users, items), bf16),
            jax.ShapeDtypeStruct((parts, steps * piece + groups, width), f32),
            jax.ShapeDtypeStruct((width, users), f32),
            jax.ShapeDtypeStruct((groups, lanes), f32),
        ],
        scratch_shapes=[
            pltpu.VMEM((2 * width, items), bf16),
            pltpu.VMEM((width, items), bf16),
            pltpu.VMEM((items, 2 * width), bf16),
            pltpu.VMEM((users, items), jnp.int32),
            pltpu.SemaphoreType.DMA((steps,)),
        ],
        compiler_params=pltpu.CompilerParams(vmem_limit_bytes=32 << 20),
        cost_estimate=cost(12 * users * items * width),
        name="block",
    )(user_rows, item_rows, pltpu.with_memory_space_constraint(prefs, pltpu.HBM), rate)


def relay_kernel(tiles_ref, out_ref):
    runs, rows, width = out_ref.shape
    piece = (tiles_ref.shape[1] - rows) // (runs - 1)
    summed = jnp.sum(tiles_ref[...], axis=0)
    for run in range(runs):
        out_ref[run, :piece, :] = summed[run * piece : (run + 1) * piece]
        out_ref[run, piece:, :] = summed[runs * piece :]


def relay(tiles, runs, groups):
    rows = tiles.shape[1] - groups
    return pl.pallas_call(
        relay_kernel,
        in_specs=[whole],
        out_specs=whole,
        out_shape=jax.ShapeDtypeStruct((runs, rows // runs + groups, lanes), f32),
        compiler_params=pltpu.CompilerParams(vmem_limit_bytes=8 << 20),
        cost_estimate=cost(1 << 20),
        name="relay",
    )(tiles)


def item_kernel(bound_scale, slab_ref, norm_ref, clip_ref, turned_ref, high_ref, low_ref, keep_ref, give_ref, pair_ref):
    width, users = turned_ref.shape
    items = high_ref.shape[1]
    groups = norm_ref.shape[0]
    bit = keep_ref.shape[1]
    tile = 2 * lanes
    first = lax.axis_index("core") == 0
    total = jnp.sum(slab_ref[:, slab_ref.shape[1] - groups :, :], axis=0)
    bound = clip_ref[...].astype(f32) * bound_scale
    factor = jnp.minimum(1.0, bound / jnp.sqrt(total * norm_ref[...] + 1e-06))
    for part in range(users // lanes):
        place = slice(part * lanes, (part + 1) * lanes)
        pair_ref[:width, place], pair_ref[width:, place] = halves(turned_ref[:, place] * factor[part : part + 1, :])
    for part in range(items // tile):
        place = slice(part * tile, (part + 1) * tile)
        tall = product(pair_ref[...], high_ref[:, place])
        summed = tall[:width] + tall[width:] + product(pair_ref[:width, :], low_ref[:, place])
        for inner in range(tile // lanes):
            rows = summed[:, inner * lanes : (inner + 1) * lanes].T
            for piece in range(lanes // (2 * bit)):
                index = (part * tile + inner * lanes) // (2 * bit) + piece
                even = rows[2 * piece * bit : (2 * piece + 1) * bit, :]
                odd = rows[(2 * piece + 1) * bit : (2 * piece + 2) * bit, :]
                keep_ref[index] = jnp.where(first, even, odd)
                give_ref[index] = jnp.where(first, odd, even)


def item_gradients(bound_scale, slab, norm, clip, turned, high, low, bit):
    users, items = high.shape
    width = turned.shape[0]

    def body(*refs):
        item_kernel(bound_scale, *refs)

    return pl.pallas_call(
        body,
        in_specs=[whole] * 6,
        out_specs=[whole] * 2,
        out_shape=[jax.ShapeDtypeStruct((items // (2 * bit), bit, width), f32)] * 2,
        scratch_shapes=[pltpu.VMEM((2 * width, users), bf16)],
        compiler_params=pltpu.CompilerParams(vmem_limit_bytes=24 << 20),
        cost_estimate=cost(6 * users * items * width),
        name="item_gradients",
    )(slab, norm, clip, turned, high, low)


def join_kernel(keep_ref, both_ref, out_ref):
    out_ref[...] = keep_ref[...] + both_ref[1 - lax.axis_index("core")]


def join(keep, both):
    return pl.pallas_call(
        join_kernel,
        in_specs=[whole] * 2,
        out_specs=whole,
        out_shape=jax.ShapeDtypeStruct(keep.shape, f32),
        compiler_params=pltpu.CompilerParams(vmem_limit_bytes=8 << 20),
        cost_estimate=cost(1 << 20),
        name="join",
    )(keep, both)


def step_of(emb, acc, gradient):
    new_acc = acc + gradient * gradient
    return emb - learn_rate * gradient / jnp.sqrt(new_acc), new_acc


def user_kernel(slab_ref, emb_ref, acc_ref, emb_out, acc_out):
    gradient = jnp.sum(slab_ref[:, : emb_ref.shape[0], :], axis=0)
    emb_out[...], acc_out[...] = step_of(emb_ref[...], acc_ref[...], gradient)


def last_kernel(tiles_ref, emb_ref, acc_ref, noise_ref, emb_out, acc_out):
    gradient = jnp.sum(tiles_ref[...], axis=0) + noise_step * noise_ref[...].astype(f32)
    emb_out[...], acc_out[...] = step_of(emb_ref[...], acc_ref[...], gradient)


def finish(body, name, tiles, emb, *rest):
    result = jax.ShapeDtypeStruct(emb.shape, f32)
    return pl.pallas_call(
        body,
        in_specs=[whole] * (2 + len(rest)),
        out_specs=[whole] * 2,
        out_shape=[result] * 2,
        compiler_params=pltpu.CompilerParams(vmem_limit_bytes=8 << 20),
        cost_estimate=cost(1 << 24),
        name=name,
    )(tiles, emb, *rest)


def exchange(value, axis):
    return lax.all_to_all(value, axis, 0, 0, tiled=True)


def from_everyone(value, axis):
    return exchange(jnp.broadcast_to(value[None], (lax.axis_size(axis), *value.shape)), axis)


def local(prefs, item_weight, clip_units, user_emb, user_acc, item_emb, item_acc, noise):
    users, items = prefs.shape
    piece, width = user_emb.shape
    bit = item_emb.shape[0]
    groups = users // lanes
    bound_scale = 0.001 * (items * lax.axis_size(item_axes) * width) ** 0.5
    user_run = from_everyone(user_emb, "run")
    item_pair = lax.all_gather(item_emb, "half")
    item_line = from_everyone(item_pair, "z").reshape(-1, bit, width)
    user_rows = lax.all_gather(user_run, "x")
    item_rows = lax.all_gather(item_line, "core")
    high, low, sent, turned, norm = block(user_rows, item_rows, prefs, item_weight.reshape(1, items))
    slab = exchange(relay(exchange(sent, "x"), lax.axis_size("run"), groups), "run")
    keep, give = item_gradients(bound_scale, slab, norm, clip_units.reshape(groups, lanes), turned, high, low, bit)
    tiles = exchange(join(keep, lax.all_gather(give, "core")), chip_axes)
    users_new = finish(user_kernel, "finish_users", slab, user_emb, user_acc)
    items_new = finish(last_kernel, "finish_items", tiles, item_emb, item_acc, noise)
    return (*users_new, *items_new)


def solution(mesh):
    fine = Mesh(mesh.devices.reshape(sizes), names)
    by_user = P(user_axes + item_axes, None)
    by_item = P(item_axes + user_axes, None)
    return jax.shard_map(
        local,
        mesh=fine,
        in_specs=(P(user_axes, item_axes), P(item_axes), P(user_axes), by_user, by_user, by_item, by_item, by_item),
        out_specs=(by_user, by_user, by_item, by_item),
        check_vma=False,
    )
```

```python
import jax
import jax.numpy as jnp
from jax import lax
from jax.experimental import pallas as pl
from jax.experimental.pallas import tpu as pltpu
from jax.sharding import Mesh, PartitionSpec as P

noise_step = 0.05
learn_rate = 0.5
lanes = 128
f32 = jnp.float32
bf16 = jnp.bfloat16

names = ("z", "half", "core", "run", "x")
sizes = (8, 2, 2, 4, 4)
user_axes = names[:3]
item_axes = names[3:]

whole = pl.BlockSpec(memory_space=pltpu.VMEM)
far = pl.BlockSpec(memory_space=pltpu.HBM)


def halves(value):
    high = value.astype(bf16)
    return high, (value - high.astype(f32)).astype(bf16)


def product(left, right):
    return jnp.dot(left, right, preferred_element_type=f32)


def cost(flops):
    return pl.CostEstimate(flops=flops, bytes_accessed=1 << 20, transcendentals=0)


def block_kernel(
    own_ref, one_ref, two_ref, three_ref, item_ref, far_ref, far_rate_ref, high_ref, low_ref, sq_ref, turned_ref, norm_ref, *more_refs
):
    *out_refs, pair_ref, rest_ref, tall_ref, prefs_ref, rate_ref, near_ref, user_ref, sum_ref, ready, gone, rated = more_refs
    parts, steps, piece, width = user_ref.shape
    mine = lax.axis_index("x")
    _, items = prefs_ref.shape
    rows = parts * piece
    tile = 2 * lanes
    blocks = [slice(step * rows, (step + 1) * rows) for step in range(steps)]
    copies = [pltpu.make_async_copy(far_ref.at[span], prefs_ref.at[span], ready.at[step]) for step, span in enumerate(blocks)]
    rates = pltpu.make_async_copy(far_rate_ref, rate_ref, rated)
    rates.start()
    for copy in copies:
        copy.start()
    stores = [pltpu.make_async_copy(near_ref.at[span], low_ref.at[span], gone.at[step]) for step, span in enumerate(blocks)]
    for shift, ref in enumerate((own_ref, one_ref, two_ref, three_ref)):
        user_ref[lax.rem(mine + parts - shift, parts)] = ref[...]
    cores, _, bit, _ = item_ref.shape
    per = lanes // (cores * bit)
    for part in range(items // lanes):
        place = slice(part * lanes, (part + 1) * lanes)
        together = [item_ref[core, part * per + line] for line in range(per) for core in range(cores)]
        value = jnp.concatenate(together, axis=0)
        high, low = halves(value)
        tall_ref[place, :width] = high
        tall_ref[place, width:] = low
        high, low = halves(value.T)
        pair_ref[:width, place] = high
        pair_ref[width:, place] = high
        rest_ref[:, place] = low
    for step, span in enumerate(blocks):
        user = user_ref[:, step].reshape(rows, width)
        user_high, user_low = halves(user)
        both = jnp.concatenate([user_high, user_low], axis=1)
        squares = jnp.zeros((rows, lanes), f32)
        if step == 0:
            rates.wait()
        copies[step].wait()
        for part in range(items // tile):
            place = slice(part * tile, (part + 1) * tile)
            predicted = product(both, pair_ref[:, place]) + product(user_high, rest_ref[:, place])
            level = prefs_ref[span, place].astype(f32)
            confidence = 2.0 + 2.0 * rate_ref[:, place] * level
            weighted = confidence * (predicted - jnp.where(level > 0, 1.0, 0.0))
            high_ref[span, place], near_ref[span, place] = halves(weighted)
            square = weighted * weighted
            squares = squares + square[:, :lanes] + square[:, lanes:]
        stores[step].start()
        for part in range(rows // lanes):
            row = step * (rows // lanes) + part
            total = squares[part * lanes : (part + 1) * lanes, :].T
            sq_ref[row : row + 1, :] = jnp.sum(total, axis=0, keepdims=True)
    for step, span in enumerate(blocks):
        user = user_ref[:, step].reshape(rows, width)
        wide = product(high_ref[span, :], tall_ref[...])
        gradient = wide[:, :width] + wide[:, width:] + product(near_ref[span, :], tall_ref[:, :width])
        for part in range(parts):
            sum_ref[part, step * piece : (step + 1) * piece, :] = gradient[part * piece : (part + 1) * piece, :]
        for part in range(rows // lanes):
            row = step * (rows // lanes) + part
            turned = user[part * lanes : (part + 1) * lanes, :].T
            turned_ref[:, row * lanes : (row + 1) * lanes] = turned
            norm_ref[row : row + 1, :] = jnp.sum(turned * turned, axis=0, keepdims=True)
    for shift, out_ref in enumerate(out_refs):
        out_ref[...] = sum_ref[lax.rem(mine + shift, parts)]
    for store in stores:
        store.wait()


def block(user_rows, item_rows, prefs, rate):
    parts = len(user_rows)
    steps, piece, width = user_rows[0].shape
    users, items = prefs.shape
    groups = users // lanes
    return pl.pallas_call(
        block_kernel,
        in_specs=[whole] * (parts + 1) + [far] * 2,
        out_specs=[whole, far] + [whole] * (3 + parts),
        out_shape=[
            jax.ShapeDtypeStruct((users, items), bf16),
            pltpu.HBM((users, items), bf16),
            jax.ShapeDtypeStruct((groups, lanes), f32),
            jax.ShapeDtypeStruct((width, users), f32),
            jax.ShapeDtypeStruct((groups, lanes), f32),
        ]
        + [jax.ShapeDtypeStruct((users // parts, width), f32)] * parts,
        scratch_shapes=[
            pltpu.VMEM((2 * width, items), bf16),
            pltpu.VMEM((width, items), bf16),
            pltpu.VMEM((items, 2 * width), bf16),
            pltpu.VMEM((users, items), jnp.int32),
            pltpu.VMEM((1, items), f32),
            pltpu.VMEM((users, items), bf16),
            pltpu.VMEM((parts, steps, piece, width), f32),
            pltpu.VMEM((parts, users // parts, width), f32),
            pltpu.SemaphoreType.DMA((steps,)),
            pltpu.SemaphoreType.DMA((steps,)),
            pltpu.SemaphoreType.DMA,
        ],
        compiler_params=pltpu.CompilerParams(vmem_limit_bytes=20 << 20),
        cost_estimate=cost(12 * users * items * width),
        name="block",
    )(*user_rows, item_rows, *(pltpu.with_memory_space_constraint(value, pltpu.HBM) for value in (prefs, rate)))


def relay_kernel(own_ref, one_ref, two_ref, three_ref, *more_refs):
    *out_refs, sum_ref = more_refs
    piece = out_refs[0].shape[0]
    sum_ref[...] = own_ref[...] + one_ref[...] + two_ref[...] + three_ref[...]
    mine = lax.axis_index("run")
    for shift, out_ref in enumerate(out_refs):
        start = pl.multiple_of(lax.rem(mine + shift, len(out_refs)) * piece, piece)
        out_ref[...] = sum_ref[pl.ds(start, piece), :]


def relay(parts):
    rows, width = parts[0].shape
    count = len(parts)
    return pl.pallas_call(
        relay_kernel,
        in_specs=[whole] * count,
        out_specs=[whole] * count,
        out_shape=[jax.ShapeDtypeStruct((rows // count, width), f32)] * count,
        scratch_shapes=[pltpu.VMEM((rows, width), f32)],
        compiler_params=pltpu.CompilerParams(vmem_limit_bytes=8 << 20),
        cost_estimate=cost(1 << 20),
        name="relay",
    )(*parts)


def item_kernel(bound_scale, all_sq_ref, norm_ref, clip_ref, turned_ref, high_ref, far_ref, keep_ref, give_ref, pair_ref, low_ref, first_ref, ready):
    width, users = turned_ref.shape
    items = high_ref.shape[1]
    bit = keep_ref.shape[1]
    tile = 2 * lanes
    first = lax.axis_index("core") == 0
    spans = [slice(part * tile, (part + 1) * tile) for part in range(users // tile)]
    copies = [pltpu.make_async_copy(far_ref.at[span], low_ref.at[span], ready.at[part]) for part, span in enumerate(spans)]
    for copy in copies:
        copy.start()
    total = jnp.sum(all_sq_ref[...], axis=0)
    bound = clip_ref[...].astype(f32) * bound_scale
    factor = jnp.minimum(1.0, bound / jnp.sqrt(total * norm_ref[...] + 1e-06))
    for part in range(users // lanes):
        place = slice(part * lanes, (part + 1) * lanes)
        pair_ref[:width, place], pair_ref[width:, place] = halves(turned_ref[:, place] * factor[part : part + 1, :])
    for part in range(items // tile):
        place = slice(part * tile, (part + 1) * tile)
        tall = product(pair_ref[...], high_ref[:, place])
        first_ref[:, place] = tall[:width] + tall[width:]
    for copy in copies:
        copy.wait()
    for part in range(items // tile):
        place = slice(part * tile, (part + 1) * tile)
        summed = first_ref[:, place] + product(pair_ref[:width, :], low_ref[:, place])
        for inner in range(tile // lanes):
            rows = summed[:, inner * lanes : (inner + 1) * lanes].T
            for piece in range(lanes // (2 * bit)):
                index = (part * tile + inner * lanes) // (2 * bit) + piece
                even = rows[2 * piece * bit : (2 * piece + 1) * bit, :]
                odd = rows[(2 * piece + 1) * bit : (2 * piece + 2) * bit, :]
                keep_ref[index] = jnp.where(first, even, odd)
                give_ref[index] = jnp.where(first, odd, even)


def item_gradients(bound_scale, all_sq, norm, clip, turned, high, low, bit):
    users, items = high.shape
    width = turned.shape[0]

    def body(*refs):
        item_kernel(bound_scale, *refs)

    return pl.pallas_call(
        body,
        in_specs=[whole] * 5 + [far],
        out_specs=[whole] * 2,
        out_shape=[jax.ShapeDtypeStruct((items // (2 * bit), bit, width), f32)] * 2,
        scratch_shapes=[
            pltpu.VMEM((2 * width, users), bf16),
            pltpu.VMEM((users, items), bf16),
            pltpu.VMEM((width, items), f32),
            pltpu.SemaphoreType.DMA((users // (2 * lanes),)),
        ],
        compiler_params=pltpu.CompilerParams(vmem_limit_bytes=12 << 20),
        cost_estimate=cost(6 * users * items * width),
        name="item_gradients",
    )(all_sq, norm, clip, turned, high, pltpu.with_memory_space_constraint(low, pltpu.HBM))


def join_kernel(keep_ref, both_ref, out_ref):
    out_ref[...] = keep_ref[...] + both_ref[1 - lax.axis_index("core")]


def join(keep, both):
    return pl.pallas_call(
        join_kernel,
        in_specs=[whole] * 2,
        out_specs=whole,
        out_shape=jax.ShapeDtypeStruct(keep.shape, f32),
        compiler_params=pltpu.CompilerParams(vmem_limit_bytes=8 << 20),
        cost_estimate=cost(1 << 20),
        name="join",
    )(keep, both)


def fold_kernel(tiles_ref, keep_ref, give_ref):
    mine = lax.axis_index("half")
    keep_ref[...] = jnp.sum(tiles_ref[:, mine], axis=0)
    give_ref[...] = jnp.sum(tiles_ref[:, 1 - mine], axis=0)


def fold(tiles):
    return pl.pallas_call(
        fold_kernel,
        in_specs=[whole],
        out_specs=[whole] * 2,
        out_shape=[jax.ShapeDtypeStruct(tiles.shape[2:], f32)] * 2,
        compiler_params=pltpu.CompilerParams(vmem_limit_bytes=8 << 20),
        cost_estimate=cost(1 << 20),
        name="fold",
    )(tiles)


def step_of(emb, acc, gradient):
    new_acc = acc + gradient * gradient
    return emb - learn_rate * gradient / jnp.sqrt(new_acc), new_acc


def finish_kernel(
    own_ref, one_ref, two_ref, three_ref, keep_ref, both_ref, user_ref, user_acc_ref, item_ref, item_acc_ref, noise_ref,
    user_out, user_acc_out, item_out, item_acc_out
):
    user_grad = own_ref[...] + one_ref[...] + two_ref[...] + three_ref[...]
    user_out[...], user_acc_out[...] = step_of(user_ref[...], user_acc_ref[...], user_grad)
    item_grad = keep_ref[...] + both_ref[1 - lax.axis_index("half")] + noise_step * noise_ref[...].astype(f32)
    item_out[...], item_acc_out[...] = step_of(item_ref[...], item_acc_ref[...], item_grad)


def finish(parts, keep, both, user_emb, user_acc, item_emb, item_acc, noise):
    user = jax.ShapeDtypeStruct(user_emb.shape, f32)
    item = jax.ShapeDtypeStruct(item_emb.shape, f32)
    return pl.pallas_call(
        finish_kernel,
        in_specs=[whole] * (7 + len(parts)),
        out_specs=[whole] * 4,
        out_shape=[user, user, item, item],
        compiler_params=pltpu.CompilerParams(vmem_limit_bytes=8 << 20),
        name="finish",
    )(*parts, keep, both, user_emb, user_acc, item_emb, item_acc, noise)


def passed_round(parts, axis):
    count = lax.axis_size(axis)
    moved = [
        lax.ppermute(part, axis, [(place, (place + shift) % count) for place in range(count)])
        for shift, part in enumerate(parts)
        if shift
    ]
    return [parts[0], *moved]


def exchange(value, axis):
    return lax.all_to_all(value, axis, 0, 0, tiled=True)


def from_everyone(value, axis):
    return exchange(jnp.broadcast_to(value[None], (lax.axis_size(axis), *value.shape)), axis)


def local(prefs, item_weight, clip_units, user_emb, user_acc, item_emb, item_acc, noise):
    users, items = prefs.shape
    _, width = user_emb.shape
    bit = item_emb.shape[0]
    groups = users // lanes
    bound_scale = 0.001 * (items * lax.axis_size(item_axes) * width) ** 0.5
    user_run = from_everyone(user_emb, "run")
    item_pair = lax.all_gather(item_emb, "half")
    item_line = from_everyone(item_pair, "z").reshape(-1, bit, width)
    user_rows = passed_round([user_run] * lax.axis_size("x"), "x")
    item_rows = lax.all_gather(item_line, "core")
    high, low, sq, turned, norm, *parts = block(user_rows, item_rows, prefs, item_weight.reshape(1, items))
    all_sq = from_everyone(sq, item_axes)
    parts = passed_round(parts, "x")
    parts = relay(parts)
    parts = passed_round(parts, "run")
    keep, give = item_gradients(bound_scale, all_sq, norm, clip_units.reshape(groups, lanes), turned, high, low, bit)
    joined = join(keep, lax.all_gather(give, "core"))
    tiles = exchange(joined.reshape(-1, 2, bit, width), "z")
    keep, give = fold(tiles)
    both = lax.all_gather(give, "half")
    return tuple(finish(parts, keep, both, user_emb, user_acc, item_emb, item_acc, noise))


def solution(mesh):
    fine = Mesh(mesh.devices.reshape(sizes), names)
    by_user = P(user_axes + item_axes, None)
    by_item = P(item_axes + user_axes, None)
    return jax.shard_map(
        local,
        mesh=fine,
        in_specs=(P(user_axes, item_axes), P(item_axes), P(user_axes), by_user, by_user, by_item, by_item, by_item),
        out_specs=(by_user, by_user, by_item, by_item),
        check_vma=False,
    )
```

```python
import jax
import jax.numpy as jnp
from jax import lax
from jax.experimental import pallas as pl
from jax.experimental.pallas import tpu as pltpu
from jax.sharding import Mesh, PartitionSpec as P

noise_step = 0.05
learn_rate = 0.5
lanes = 128
f32 = jnp.float32
bf16 = jnp.bfloat16

names = ("z", "half", "core", "run", "x")
sizes = (8, 2, 2, 4, 4)
user_axes = names[:3]
item_axes = names[3:]

whole = pl.BlockSpec(memory_space=pltpu.VMEM)
far = pl.BlockSpec(memory_space=pltpu.HBM)


def halves(value):
    high = value.astype(bf16)
    return high, (value - high.astype(f32)).astype(bf16)


def product(left, right):
    return jnp.dot(left, right, preferred_element_type=f32)


def cost(flops):
    return pl.CostEstimate(flops=flops, bytes_accessed=1 << 20, transcendentals=0)


def block_kernel(
    own_ref, one_ref, two_ref, three_ref, item_ref, far_ref, far_rate_ref, high_ref, low_ref, all_sq_ref, turned_ref, norm_ref, *more_refs
):
    *out_refs, pair_ref, rest_ref, tall_ref, prefs_ref, rate_ref, near_ref, user_ref, sum_ref, copies_ref, ready, gone, rated, spread, sent = more_refs
    parts, steps, piece, width = user_ref.shape
    mine = lax.axis_index("x")
    _, items = prefs_ref.shape
    rows = parts * piece
    tile = 2 * lanes
    blocks = [slice(step * rows, (step + 1) * rows) for step in range(steps)]
    copies = [pltpu.make_async_copy(far_ref.at[span], prefs_ref.at[span], ready.at[step]) for step, span in enumerate(blocks)]
    rates = pltpu.make_async_copy(far_rate_ref, rate_ref, rated)
    rates.start()
    for copy in copies:
        copy.start()
    stores = [pltpu.make_async_copy(near_ref.at[span], low_ref.at[span], gone.at[step]) for step, span in enumerate(blocks)]
    for shift, ref in enumerate((own_ref, one_ref, two_ref, three_ref)):
        user_ref[lax.rem(mine + parts - shift, parts)] = ref[...]
    cores, _, bit, _ = item_ref.shape
    per = lanes // (cores * bit)
    for part in range(items // lanes):
        place = slice(part * lanes, (part + 1) * lanes)
        together = [item_ref[core, part * per + line] for line in range(per) for core in range(cores)]
        value = jnp.concatenate(together, axis=0)
        high, low = halves(value)
        tall_ref[place, :width] = high
        tall_ref[place, width:] = low
        high, low = halves(value.T)
        pair_ref[:width, place] = high
        pair_ref[width:, place] = high
        rest_ref[:, place] = low
    for step, span in enumerate(blocks):
        user = user_ref[:, step].reshape(rows, width)
        user_high, user_low = halves(user)
        both = jnp.concatenate([user_high, user_low], axis=1)
        squares = jnp.zeros((rows, lanes), f32)
        if step == 0:
            rates.wait()
        copies[step].wait()
        for part in range(items // tile):
            place = slice(part * tile, (part + 1) * tile)
            predicted = product(both, pair_ref[:, place]) + product(user_high, rest_ref[:, place])
            level = prefs_ref[span, place].astype(f32)
            confidence = 2.0 + 2.0 * rate_ref[:, place] * level
            weighted = confidence * (predicted - jnp.where(level > 0, 1.0, 0.0))
            high_ref[span, place], near_ref[span, place] = halves(weighted)
            square = weighted * weighted
            squares = squares + square[:, :lanes] + square[:, lanes:]
        stores[step].start()
        for part in range(rows // lanes):
            row = step * (rows // lanes) + part
            total = squares[part * lanes : (part + 1) * lanes, :].T
            sums = jnp.sum(total, axis=0, keepdims=True)
            for peer in range(copies_ref.shape[0]):
                copies_ref[peer, row : row + 1, :] = sums
        wide = product(high_ref[span, :], tall_ref[...])
        gradient = wide[:, :width] + wide[:, width:] + product(near_ref[span, :], tall_ref[:, :width])
        for part in range(parts):
            sum_ref[part, step * piece : (step + 1) * piece, :] = gradient[part * piece : (part + 1) * piece, :]
    stores.append(pltpu.make_async_copy(copies_ref, all_sq_ref, spread))
    for shift in range(1, parts):
        stores.append(pltpu.make_async_copy(sum_ref.at[lax.rem(mine + shift, parts)], out_refs[shift], sent.at[shift - 1]))
    for store in stores[steps:]:
        store.start()
    out_refs[0][...] = sum_ref[mine]
    for step in range(steps):
        user = user_ref[:, step].reshape(rows, width)
        for part in range(rows // lanes):
            row = step * (rows // lanes) + part
            turned = user[part * lanes : (part + 1) * lanes, :].T
            turned_ref[:, row * lanes : (row + 1) * lanes] = turned
            norm_ref[row : row + 1, :] = jnp.sum(turned * turned, axis=0, keepdims=True)
    for store in stores:
        store.wait()


def block(user_rows, item_rows, prefs, rate):
    parts = len(user_rows)
    peers = lax.axis_size(item_axes)
    steps, piece, width = user_rows[0].shape
    users, items = prefs.shape
    groups = users // lanes
    return pl.pallas_call(
        block_kernel,
        in_specs=[whole] * (parts + 1) + [far] * 2,
        out_specs=[whole, far, far] + [whole] * 3 + [far] * (parts - 1),
        out_shape=[
            jax.ShapeDtypeStruct((users, items), bf16),
            pltpu.HBM((users, items), bf16),
            pltpu.HBM((peers, groups, lanes), f32),
            jax.ShapeDtypeStruct((width, users), f32),
            jax.ShapeDtypeStruct((groups, lanes), f32),
        ]
        + [jax.ShapeDtypeStruct((users // parts, width), f32)]
        + [pltpu.HBM((users // parts, width), f32)] * (parts - 1),
        scratch_shapes=[
            pltpu.VMEM((2 * width, items), bf16),
            pltpu.VMEM((width, items), bf16),
            pltpu.VMEM((items, 2 * width), bf16),
            pltpu.VMEM((users, items), jnp.int32),
            pltpu.VMEM((1, items), f32),
            pltpu.VMEM((users, items), bf16),
            pltpu.VMEM((parts, steps, piece, width), f32),
            pltpu.VMEM((parts, users // parts, width), f32),
            pltpu.VMEM((peers, groups, lanes), f32),
            pltpu.SemaphoreType.DMA((steps,)),
            pltpu.SemaphoreType.DMA((steps,)),
            pltpu.SemaphoreType.DMA,
            pltpu.SemaphoreType.DMA,
            pltpu.SemaphoreType.DMA((parts - 1,)),
        ],
        compiler_params=pltpu.CompilerParams(vmem_limit_bytes=20 << 20),
        cost_estimate=cost(12 * users * items * width),
        name="block",
    )(*user_rows, item_rows, *(pltpu.with_memory_space_constraint(value, pltpu.HBM) for value in (prefs, rate)))


def relay_kernel(own_ref, one_ref, two_ref, three_ref, *more_refs):
    *out_refs, sum_ref = more_refs
    piece = out_refs[0].shape[0]
    sum_ref[...] = own_ref[...] + one_ref[...] + two_ref[...] + three_ref[...]
    mine = lax.axis_index("run")
    for shift, out_ref in enumerate(out_refs):
        start = pl.multiple_of(lax.rem(mine + shift, len(out_refs)) * piece, piece)
        out_ref[...] = sum_ref[pl.ds(start, piece), :]


def relay(parts):
    rows, width = parts[0].shape
    count = len(parts)
    return pl.pallas_call(
        relay_kernel,
        in_specs=[whole] * count,
        out_specs=[whole] * count,
        out_shape=[jax.ShapeDtypeStruct((rows // count, width), f32)] * count,
        scratch_shapes=[pltpu.VMEM((rows, width), f32)],
        compiler_params=pltpu.CompilerParams(vmem_limit_bytes=8 << 20),
        cost_estimate=cost(1 << 20),
        name="relay",
    )(*parts)


def item_kernel(bound_scale, all_sq_ref, norm_ref, clip_ref, turned_ref, high_ref, far_ref, keep_ref, give_ref, pair_ref, low_ref, first_ref, ready):
    width, users = turned_ref.shape
    items = high_ref.shape[1]
    bit = keep_ref.shape[1]
    tile = 2 * lanes
    first = lax.axis_index("core") == 0
    spans = [slice(part * tile, (part + 1) * tile) for part in range(users // tile)]
    copies = [pltpu.make_async_copy(far_ref.at[span], low_ref.at[span], ready.at[part]) for part, span in enumerate(spans)]
    for copy in copies:
        copy.start()
    total = jnp.sum(all_sq_ref[...], axis=0)
    bound = clip_ref[...].astype(f32) * bound_scale
    factor = jnp.minimum(1.0, bound / jnp.sqrt(total * norm_ref[...] + 1e-06))
    for part in range(users // lanes):
        place = slice(part * lanes, (part + 1) * lanes)
        pair_ref[:width, place], pair_ref[width:, place] = halves(turned_ref[:, place] * factor[part : part + 1, :])
    for part in range(items // tile):
        place = slice(part * tile, (part + 1) * tile)
        tall = product(pair_ref[...], high_ref[:, place])
        first_ref[:, place] = tall[:width] + tall[width:]
    for span, copy in zip(spans[:-1], copies[:-1]):
        copy.wait()
        for part in range(items // tile):
            place = slice(part * tile, (part + 1) * tile)
            first_ref[:, place] += product(pair_ref[:width, span], low_ref[span, place])
    last = spans[-1]
    copies[-1].wait()
    for part in range(items // tile):
        place = slice(part * tile, (part + 1) * tile)
        summed = first_ref[:, place] + product(pair_ref[:width, last], low_ref[last, place])
        for inner in range(tile // lanes):
            rows = summed[:, inner * lanes : (inner + 1) * lanes].T
            for piece in range(lanes // (2 * bit)):
                index = (part * tile + inner * lanes) // (2 * bit) + piece
                even = rows[2 * piece * bit : (2 * piece + 1) * bit, :]
                odd = rows[(2 * piece + 1) * bit : (2 * piece + 2) * bit, :]
                keep_ref[index] = jnp.where(first, even, odd)
                give_ref[index] = jnp.where(first, odd, even)


def item_gradients(bound_scale, all_sq, norm, clip, turned, high, low, bit):
    users, items = high.shape
    width = turned.shape[0]

    def body(*refs):
        item_kernel(bound_scale, *refs)

    return pl.pallas_call(
        body,
        in_specs=[whole] * 5 + [far],
        out_specs=[whole] * 2,
        out_shape=[jax.ShapeDtypeStruct((items // (2 * bit), bit, width), f32)] * 2,
        scratch_shapes=[
            pltpu.VMEM((2 * width, users), bf16),
            pltpu.VMEM((users, items), bf16),
            pltpu.VMEM((width, items), f32),
            pltpu.SemaphoreType.DMA((users // (2 * lanes),)),
        ],
        compiler_params=pltpu.CompilerParams(vmem_limit_bytes=12 << 20),
        cost_estimate=cost(6 * users * items * width),
        name="item_gradients",
    )(all_sq, norm, clip, turned, high, pltpu.with_memory_space_constraint(low, pltpu.HBM))


def join_kernel(keep_ref, both_ref, out_ref):
    out_ref[...] = keep_ref[...] + both_ref[1 - lax.axis_index("core")]


def join(keep, both):
    return pl.pallas_call(
        join_kernel,
        in_specs=[whole] * 2,
        out_specs=whole,
        out_shape=jax.ShapeDtypeStruct(keep.shape, f32),
        compiler_params=pltpu.CompilerParams(vmem_limit_bytes=8 << 20),
        cost_estimate=cost(1 << 20),
        name="join",
    )(keep, both)


def fold_kernel(tiles_ref, keep_ref, give_ref):
    mine = lax.axis_index("half")
    keep_ref[...] = jnp.sum(tiles_ref[:, mine], axis=0)
    give_ref[...] = jnp.sum(tiles_ref[:, 1 - mine], axis=0)


def fold(tiles):
    return pl.pallas_call(
        fold_kernel,
        in_specs=[whole],
        out_specs=[whole] * 2,
        out_shape=[jax.ShapeDtypeStruct(tiles.shape[2:], f32)] * 2,
        compiler_params=pltpu.CompilerParams(vmem_limit_bytes=8 << 20),
        cost_estimate=cost(1 << 20),
        name="fold",
    )(tiles)


def step_of(emb, acc, gradient):
    new_acc = acc + gradient * gradient
    return emb - learn_rate * gradient / jnp.sqrt(new_acc), new_acc


def finish_kernel(
    own_ref, one_ref, two_ref, three_ref, keep_ref, both_ref, user_ref, user_acc_ref, item_ref, item_acc_ref, noise_ref,
    user_out, user_acc_out, item_out, item_acc_out
):
    user_grad = own_ref[...] + one_ref[...] + two_ref[...] + three_ref[...]
    user_out[...], user_acc_out[...] = step_of(user_ref[...], user_acc_ref[...], user_grad)
    item_grad = keep_ref[...] + both_ref[1 - lax.axis_index("half")] + noise_step * noise_ref[...].astype(f32)
    item_out[...], item_acc_out[...] = step_of(item_ref[...], item_acc_ref[...], item_grad)


def finish(parts, keep, both, user_emb, user_acc, item_emb, item_acc, noise):
    user = jax.ShapeDtypeStruct(user_emb.shape, f32)
    item = jax.ShapeDtypeStruct(item_emb.shape, f32)
    return pl.pallas_call(
        finish_kernel,
        in_specs=[whole] * (7 + len(parts)),
        out_specs=[whole] * 4,
        out_shape=[user, user, item, item],
        compiler_params=pltpu.CompilerParams(vmem_limit_bytes=8 << 20),
        name="finish",
    )(*parts, keep, both, user_emb, user_acc, item_emb, item_acc, noise)


def passed_round(parts, axis):
    count = lax.axis_size(axis)
    moved = [
        lax.ppermute(part, axis, [(place, (place + shift) % count) for place in range(count)])
        for shift, part in enumerate(parts)
        if shift
    ]
    return [parts[0], *moved]


def exchange(value, axis):
    return lax.all_to_all(value, axis, 0, 0, tiled=True)


def from_everyone(value, axis):
    return exchange(jnp.broadcast_to(value[None], (lax.axis_size(axis), *value.shape)), axis)


def local(prefs, item_weight, clip_units, user_emb, user_acc, item_emb, item_acc, noise):
    users, items = prefs.shape
    _, width = user_emb.shape
    bit = item_emb.shape[0]
    groups = users // lanes
    bound_scale = 0.001 * (items * lax.axis_size(item_axes) * width) ** 0.5
    user_run = from_everyone(user_emb, "run")
    item_pair = lax.all_gather(item_emb, "half")
    item_line = from_everyone(item_pair, "z").reshape(-1, bit, width)
    user_rows = passed_round([user_run] * lax.axis_size("x"), "x")
    item_rows = lax.all_gather(item_line, "core")
    high, low, sq, turned, norm, *parts = block(user_rows, item_rows, prefs, item_weight.reshape(1, items))
    all_sq = exchange(sq, item_axes)
    parts = passed_round(parts, "x")
    parts = relay(parts)
    parts = passed_round(parts, "run")
    keep, give = item_gradients(bound_scale, all_sq, norm, clip_units.reshape(groups, lanes), turned, high, low, bit)
    joined = join(keep, lax.all_gather(give, "core"))
    tiles = exchange(joined.reshape(-1, 2, bit, width), "z")
    keep, give = fold(tiles)
    both = lax.all_gather(give, "half")
    return tuple(finish(parts, keep, both, user_emb, user_acc, item_emb, item_acc, noise))


def solution(mesh):
    fine = Mesh(mesh.devices.reshape(sizes), names)
    by_user = P(user_axes + item_axes, None)
    by_item = P(item_axes + user_axes, None)
    return jax.shard_map(
        local,
        mesh=fine,
        in_specs=(P(user_axes, item_axes), P(item_axes), P(user_axes), by_user, by_user, by_item, by_item, by_item),
        out_specs=(by_user, by_user, by_item, by_item),
        check_vma=False,
    )
```
